128 devices in a mesh: batch: 16 (over y_hi, x, core), shard: 8 (over z, y_lo).
Axes of the slice: x: 4, y: 4 (y_hi: 2, y_lo: 2; y = y_hi * 2 + y_lo), z: 4, core: 2. Of those that a mesh axis runs over, the one named last changes fastest.
Arguments:
- particles: float32 [32768, 1024], P(('batch', 'shard')), may hold values from -48 to 48
- batch_of: int32 [2, 32768], P(None, ('batch', 'shard')), may hold values from 0 to 15, as said below
- mixture_means: float32 [16, 1024], replicated, may hold values from -3 to 3
- log_weights: float32 [16], replicated, may hold values from -2 to 2
Outputs:
- moved: float32 [32768, 1024], P(('batch', 'shard'))
The draws below stay inside these ranges and needn't reach their ends.
Inputs may be any that keep to these rules, and one draw needn't show every extreme that they name: `batch_of`: in each iteration, the 256 particles of one device hold every batch number equally often, 256 / 16 times each.
All inputs are finite; a program needn't handle non-finite values.
Results may differ from the reference program's by a relative error of at most 0.00011.
Values sent between devices are 32-bit elements; how exact they have to be, the bound alone decides.
No kernel may reach another device: no remote copies, remote signals or barrier semaphores. Data moves between devices by JAX's collectives and lax.ppermute only.
A program may use at most 64 MiB of HBM per device.

```python
import jax
import jax.numpy as jnp
from jax import lax

D = 1024
COMPONENTS = 16
ITERS = 2
P_DEV = 256
BATCHES = 16
BATCH_ROWS = 2048
PARTICLES = 32768


def draw_particles(key, part):
    first, second = jax.random.split(key, 2)
    ranks = jax.random.permutation(second, D).astype(jnp.float32) + 1.0
    harmonic = jnp.sum(1.0 / (jnp.arange(D, dtype=jnp.float32) + 1.0))
    column_scale = jnp.sqrt(D / (harmonic * ranks))
    points = jax.random.normal(first, (PARTICLES, D), jnp.float32) * column_scale[None, :]
    return jnp.clip(points, -48.0, 48.0)


def draw_batch_of(key, part):
    devices = PARTICLES // P_DEV
    ranks = jax.random.randint(key, (ITERS, devices, P_DEV), 0, 2 ** 20) * P_DEV + jnp.arange(P_DEV, dtype=jnp.int32)
    ordering = jnp.argsort(ranks, axis=2, stable=True)
    return (ordering % BATCHES).reshape(ITERS, PARTICLES).astype(jnp.int32)


def gaussian(key, extent, width, most, kind=jnp.bfloat16):
    return jnp.clip(width * jax.random.normal(key, extent, jnp.float32), -most, most).astype(kind)


def setup_inputs(seed: int = 0) -> dict:
    streams_of = jax.random.split(jax.random.key(seed), 5)
    return {
        "particles": draw_particles(jax.random.fold_in(streams_of[4], 71), 0),
        "batch_of": draw_batch_of(jax.random.fold_in(streams_of[4], 71), 0),
        "mixture_means": gaussian(streams_of[2], (COMPONENTS, D), 0.5, 3.0, jnp.float32),
        "log_weights": jnp.clip(jax.random.uniform(streams_of[3], (COMPONENTS,), jnp.float32, -2.0, 2.0), -2.0, 2.0),
    }


variance = 4.0
step_size = 32.0


def mixture_score(points, mixture_means, log_weights):
    squares = jnp.sum(points * points, axis=1, keepdims=True)
    crossed = jnp.dot(points, mixture_means.T, precision=lax.Precision.HIGHEST, preferred_element_type=jnp.float32)
    centre_sq = jnp.sum(mixture_means * mixture_means, axis=1)
    logits = log_weights[None, :] - (squares - 2.0 * crossed + centre_sq[None, :]) / (2.0 * variance)
    weights_mix = jax.nn.softmax(logits, axis=1)
    pulled = jnp.dot(weights_mix, mixture_means, precision=lax.Precision.HIGHEST, preferred_element_type=jnp.float32)
    return (pulled - points) / variance


def group_drift(group, mixture_means, log_weights):
    scores = mixture_score(group, mixture_means, log_weights)
    squares = jnp.sum(group * group, axis=1)
    crossed = jnp.dot(group, group.T, precision=lax.Precision.HIGHEST, preferred_element_type=jnp.float32)
    kernel = jnp.exp(-(squares[:, None] + squares[None, :] - 2.0 * crossed) * (2.0 / D))
    acc_score = jnp.dot(kernel, scores, precision=lax.Precision.HIGHEST, preferred_element_type=jnp.float32)
    acc_point = jnp.dot(kernel, group, precision=lax.Precision.HIGHEST, preferred_element_type=jnp.float32)
    kernel_sum = jnp.sum(kernel, axis=1)
    return (acc_score + (4.0 / D) * (group * kernel_sum[:, None] - acc_point)) / BATCH_ROWS


def reference(particles, batch_of, mixture_means, log_weights):
    current = particles
    for iteration in range(ITERS):
        ordering = jnp.argsort(batch_of[iteration], stable=True).astype(jnp.int32)
        grouped = current[ordering].reshape(BATCHES, BATCH_ROWS, D)
        moved = lax.map(lambda group: group + step_size * group_drift(group, mixture_means, log_weights), grouped)
        current = jnp.zeros_like(current).at[ordering].set(moved.reshape(PARTICLES, D))
    return current
```

```python
import jax
import jax.numpy as jnp
from jax import lax
from jax.sharding import Mesh
from jax.sharding import PartitionSpec as P

GROUPS = 16
variance = 4.0
step_size = 32.0
HI = lax.Precision.HIGHEST


def device_of(x, y, z, c):
    return ((((y // 2) * 4 + x) * 2 + c) * 4 + z) * 2 + y % 2


def plane_groups():
    columns = [(x, y) for x in range(4) for y in range(4)]
    return [
        [device_of(x, y, z, c) for x, y in (columns if c == 0 else columns[::-1])]
        for z in range(4)
        for c in range(2)
    ]


def column_groups():
    return [
        [device_of(x, y, z, c) for c in range(2) for z in range(4)]
        for x in range(4)
        for y in range(4)
    ]


def dot(a, b, dims):
    return lax.dot_general(a, b, (dims, ((), ())), precision=HI, preferred_element_type=jnp.float32)


def exchange(rows):
    count, width = rows.shape
    return lax.all_to_all(
        rows.reshape(GROUPS, count // GROUPS, width),
        "d",
        split_axis=0,
        concat_axis=0,
        axis_index_groups=plane_groups(),
        tiled=True,
    ).reshape(count, width)


def kernel_terms(own, own_sq, others, means, log_weights):
    width = own.shape[1]
    other_sq = jnp.sum(others * others, axis=1)
    crossed = dot(own, others, ((1,), (1,)))
    kernel = jnp.exp(-(own_sq[:, None] + other_sq[None, :] - 2.0 * crossed) * (2.0 / width))
    centre_sq = jnp.sum(means * means, axis=1)
    pulls = dot(means, others, ((1,), (1,)))
    logits = log_weights[:, None] - (other_sq[None, :] - 2.0 * pulls + centre_sq[:, None]) / (
        2.0 * variance
    )
    mix = jax.nn.softmax(logits, axis=0)
    return (
        dot(kernel, others, ((1,), (0,))),
        dot(kernel, mix, ((1,), (1,))),
        jnp.sum(kernel, axis=1),
    )


def positions(batch, core):
    count = batch.shape[0]
    group = jnp.where(core == 0, batch, GROUPS - 1 - batch)
    key = group * count + lax.iota(jnp.int32, count)
    place = jnp.sum((key[None, :] < key[:, None]).astype(jnp.int32), axis=1)
    ids = lax.iota(jnp.int32, count)
    row = jnp.sum(jnp.where(place[None, :] == ids[:, None], ids[None, :], 0), axis=1)
    return place, row


def take(rows, index):
    return rows.at[index].get(mode="promise_in_bounds", unique_indices=True)


def shards(particles, batch_of, means, log_weights):
    count, width = particles.shape
    core = (lax.axis_index("d") // 8) % 2
    current = particles
    for iteration in range(batch_of.shape[0]):
        place, row = positions(batch_of[iteration], core)
        own = exchange(take(current, row))
        own_sq = jnp.sum(own * own, axis=1)
        members = lax.all_gather(
            own, "d", axis=0, axis_index_groups=column_groups(), tiled=True
        )
        point, mixed, total = kernel_terms(own, own_sq, members, means, log_weights)
        score = (dot(mixed, means, ((1,), (0,))) - point) / variance
        drift = (score + 4.0 / width * (own * total[:, None] - point)) / members.shape[0]
        returned = exchange(own + step_size * drift)
        current = take(returned, place)
    return current


def solution(mesh):
    flat = Mesh(mesh.devices.reshape(-1), ("d",))
    return jax.shard_map(
        shards,
        mesh=flat,
        in_specs=(P("d", None), P(None, "d"), P(), P()),
        out_specs=P("d", None),
        check_vma=False,
    )
```

```python
import jax
import jax.numpy as jnp
from jax import lax
from jax.sharding import Mesh
from jax.sharding import PartitionSpec as P

GROUPS = 16
variance = 4.0
step_size = 32.0
HI = lax.Precision.HIGHEST


def device_of(x, y, z, c):
    return ((((y // 2) * 4 + x) * 2 + c) * 4 + z) * 2 + y % 2


def plane_groups():
    columns = [(x, y if x % 2 == 0 else 3 - y) for x in range(4) for y in range(4)]
    return [
        [device_of(x, y, z, c) for x, y in (columns if c == 0 else columns[::-1])]
        for z in range(4)
        for c in range(2)
    ]


def along_z(step):
    return [
        (device_of(x, y, z, c), device_of(x, y, (z + step) % 4, c))
        for x in range(4)
        for y in range(4)
        for z in range(4)
        for c in range(2)
    ]


def other_core():
    return [
        (device_of(x, y, z, c), device_of(x, y, z, 1 - c))
        for x in range(4)
        for y in range(4)
        for z in range(4)
        for c in range(2)
    ]


def up(rows):
    return lax.ppermute(rows, "d", along_z(1))


def down(rows):
    return lax.ppermute(rows, "d", along_z(3))


def swap(rows):
    return lax.ppermute(rows, "d", other_core())


def dot(a, b, dims):
    return lax.dot_general(a, b, (dims, ((), ())), precision=HI, preferred_element_type=jnp.float32)


def exchange(rows):
    count, width = rows.shape
    return lax.all_to_all(
        rows.reshape(GROUPS, count // GROUPS, width),
        "d",
        split_axis=0,
        concat_axis=0,
        axis_index_groups=plane_groups(),
        tiled=True,
    ).reshape(count, width)


def kernel_terms(own, own_sq, others, means, log_weights):
    count, width = own.shape
    other_sq = jnp.sum(others * others, axis=1)
    crossed = dot(jnp.concatenate([own, means], axis=0), others, ((1,), (1,)))
    kernel = jnp.exp(
        -(own_sq[:, None] + other_sq[None, :] - 2.0 * crossed[:count]) * (2.0 / width)
    )
    centre_sq = jnp.sum(means * means, axis=1)
    logits = log_weights[:, None] - (
        other_sq[None, :] - 2.0 * crossed[count:] + centre_sq[:, None]
    ) / (2.0 * variance)
    mix = jax.nn.softmax(logits, axis=0)
    return (
        dot(kernel, others, ((1,), (0,))),
        dot(kernel, mix, ((1,), (1,))),
        jnp.sum(kernel, axis=1),
    )


def positions(batch, core):
    count = batch.shape[0]
    group = jnp.where(core == 0, batch, GROUPS - 1 - batch)
    key = group * count + lax.iota(jnp.int32, count)
    place = jnp.sum((key[None, :] < key[:, None]).astype(jnp.int32), axis=1)
    ids = lax.iota(jnp.int32, count)
    row = jnp.sum(jnp.where(place[None, :] == ids[:, None], ids[None, :], 0), axis=1)
    return place, row


def take(rows, index):
    return rows.at[index].get(mode="promise_in_bounds", unique_indices=True)


def shards(particles, batch_of, means, log_weights):
    count, width = particles.shape
    core = (lax.axis_index("d") // 8) % 2
    current = particles
    for iteration in range(batch_of.shape[0]):
        place, row = positions(batch_of[iteration], core)
        own = exchange(take(current, row))
        own_sq = jnp.sum(own * own, axis=1)
        low, high = own[: count // 2], own[count // 2 :]
        from_below, from_above = up(low), down(high)
        rest_below, rest_above = up(high), down(low)
        beside = swap(own)
        across = jnp.concatenate([up(from_below), down(from_above)], axis=0)
        near = jnp.concatenate([from_below, from_above], axis=0)
        rest = jnp.concatenate([rest_below, rest_above], axis=0)
        blocks = [own, beside, near, swap(near), rest, swap(rest), across, swap(across)]
        terms = [kernel_terms(own, own_sq, block, means, log_weights) for block in blocks]
        point, mixed, total = [sum(part[1:], part[0]) for part in zip(*terms)]
        score = (dot(mixed, means, ((1,), (0,))) - point) / variance
        drift = (score + 4.0 / width * (own * total[:, None] - point)) / (count * len(blocks))
        returned = exchange(own + step_size * drift)
        current = take(returned, place)
    return current


def solution(mesh):
    flat = Mesh(mesh.devices.reshape(-1), ("d",))
    return jax.shard_map(
        shards,
        mesh=flat,
        in_specs=(P("d", None), P(None, "d"), P(), P()),
        out_specs=P("d", None),
        check_vma=False,
    )
```

```python
import functools

import jax
import jax.numpy as jnp
from jax import lax
from jax.experimental import pallas as pl
from jax.experimental.pallas import tpu as pltpu
from jax.sharding import Mesh
from jax.sharding import PartitionSpec as P

GROUPS = 16
variance = 4.0
step_size = 32.0
HI = lax.Precision.HIGHEST


def device_of(x, y, z, c):
    return ((((y // 2) * 4 + x) * 2 + c) * 4 + z) * 2 + y % 2


def plane_groups():
    columns = [(x, y if x % 2 == 0 else 3 - y) for x in range(4) for y in range(4)]
    return [
        [device_of(x, y, z, c) for x, y in (columns if c == 0 else columns[::-1])]
        for z in range(4)
        for c in range(2)
    ]


def along_z(step):
    return [
        (device_of(x, y, z, c), device_of(x, y, (z + step) % 4, c))
        for x in range(4)
        for y in range(4)
        for z in range(4)
        for c in range(2)
    ]


def other_core():
    return [
        (device_of(x, y, z, c), device_of(x, y, z, 1 - c))
        for x in range(4)
        for y in range(4)
        for z in range(4)
        for c in range(2)
    ]


def send(rows, pairs):
    return lax.ppermute(rows, "d", pairs)


def exchange(rows):
    count, width = rows.shape
    return lax.all_to_all(
        rows.reshape(GROUPS, count // GROUPS, width),
        "d",
        split_axis=0,
        concat_axis=0,
        axis_index_groups=plane_groups(),
        tiled=True,
    ).reshape(count, width)


def dot(a, b, dims):
    return lax.dot_general(a, b, (dims, ((), ())), precision=HI, preferred_element_type=jnp.float32)


def terms_body(blocks, first, members, *refs):
    own_ref, means_ref, log_ref = refs[:3]
    refs = refs[3:]
    rows = refs[: sum(blocks)]
    refs = refs[sum(blocks) :]
    own = own_ref[...]
    means = means_ref[...]
    count, width = own.shape
    scale = 2.0 / width
    own_sq = jnp.sum(own * own, axis=1, keepdims=True)
    centre_sq = jnp.sum(means * means, axis=1, keepdims=True)
    left = jnp.concatenate([own, means], axis=0)
    point, mixed = (None, None) if first else (refs[0][...], refs[1][...])
    at = 0
    for parts in blocks:
        pieces = [ref[...] for ref in rows[at : at + parts]]
        at += parts
        block = pieces[0] if parts == 1 else jnp.concatenate(pieces, axis=0)
        crossed = dot(left, block, ((1,), (1,)))
        sq = jnp.sum(block * block, axis=1, keepdims=True)
        sq = jnp.broadcast_to(sq, (sq.shape[0], 128)).T[:1]
        kernel = jnp.exp(-(own_sq + sq - 2.0 * crossed[:count]) * scale)
        logits = log_ref[...] - (sq - 2.0 * crossed[count:] + centre_sq) / (2.0 * variance)
        weights = jnp.exp(logits - jnp.max(logits, axis=0, keepdims=True))
        weights = weights / jnp.sum(weights, axis=0, keepdims=True)
        columns = jnp.concatenate([weights, jnp.ones_like(weights)], axis=0)
        add_point = dot(kernel, block, ((1,), (0,)))
        add_mixed = dot(kernel, columns, ((1,), (1,)))
        point = add_point if point is None else point + add_point
        mixed = add_mixed if mixed is None else mixed + add_mixed
    if members:
        components = means.shape[0]
        pulled = dot(mixed[:, :components], means, ((1,), (0,)))
        total = mixed[:, components : components + 1]
        drift = ((pulled - point) / variance + 4.0 / width * (own * total - point)) / members
        refs[-1][...] = own + step_size * drift
    else:
        refs[-2][...] = point
        refs[-1][...] = mixed


def terms(own, means, log_weights, blocks, sums=None, members=0):
    count, width = own.shape
    components = means.shape[0]
    rows = [piece for block in blocks for piece in block]
    operands = [own, means, log_weights[:, None], *rows, *(sums or ())]
    wide = jax.ShapeDtypeStruct((count, width), jnp.float32)
    narrow = jax.ShapeDtypeStruct((count, 2 * components), jnp.float32)
    vmem = pl.BlockSpec(memory_space=pltpu.VMEM)
    alias = {}
    if sums:
        base = len(operands) - 2
        alias = {base: 0} if members else {base: 0, base + 1: 1}
    total_rows = sum(piece.shape[0] for piece in rows)
    return pl.pallas_call(
        functools.partial(terms_body, [len(b) for b in blocks], sums is None, members),
        out_shape=wide if members else (wide, narrow),
        in_specs=[vmem] * len(operands),
        out_specs=vmem if members else (vmem, vmem),
        input_output_aliases=alias,
        compiler_params=pltpu.CompilerParams(vmem_limit_bytes=40 * 2**20),
        cost_estimate=pl.CostEstimate(
            flops=24 * count * total_rows * width,
            transcendentals=count * total_rows,
            bytes_accessed=4 * width * (total_rows + 3 * count),
        ),
    )(*operands)


def positions(batch, core):
    count = batch.shape[0]
    group = jnp.where(core == 0, batch, GROUPS - 1 - batch)
    key = group * count + lax.iota(jnp.int32, count)
    place = jnp.sum((key[None, :] < key[:, None]).astype(jnp.int32), axis=1)
    ids = lax.iota(jnp.int32, count)
    row = jnp.sum(jnp.where(place[None, :] == ids[:, None], ids[None, :], 0), axis=1)
    return place, row


def take(rows, index):
    return rows.at[index].get(mode="promise_in_bounds", unique_indices=True)


def shards(particles, batch_of, means, log_weights):
    count, _ = particles.shape
    core = (lax.axis_index("d") // 8) % 2
    above, below, beside = along_z(1), along_z(3), other_core()
    current = particles
    for iteration in range(batch_of.shape[0]):
        place, row = positions(batch_of[iteration], core)
        own = exchange(take(current, row))
        low, high = own[: count // 2], own[count // 2 :]
        near = [send(low, above), send(high, below)]
        rest = [send(high, above), send(low, below)]
        side = send(own, beside)
        far = [send(near[0], above), send(near[1], below)]
        near_side = [send(rows, beside) for rows in near]
        rest_side = [send(rows, beside) for rows in rest]
        far_side = [send(rows, beside) for rows in far]
        sums = terms(own, means, log_weights, [[own], [side]])
        sums = terms(own, means, log_weights, [near, near_side], sums)
        sums = terms(own, means, log_weights, [rest, rest_side], sums)
        moved = terms(own, means, log_weights, [far, far_side], sums, members=8 * count)
        current = take(exchange(moved), place)
    return current


def solution(mesh):
    flat = Mesh(mesh.devices.reshape(-1), ("d",))
    return jax.shard_map(
        shards,
        mesh=flat,
        in_specs=(P("d", None), P(None, "d"), P(), P()),
        out_specs=P("d", None),
        check_vma=False,
    )
```

```python
import functools

import jax
import jax.numpy as jnp
from jax import lax
from jax.experimental import pallas as pl
from jax.experimental.pallas import tpu as pltpu
from jax.sharding import Mesh
from jax.sharding import PartitionSpec as P

GROUPS = 16
variance = 4.0
step_size = 32.0


def device_of(x, y, z, c):
    return ((((y // 2) * 4 + x) * 2 + c) * 4 + z) * 2 + y % 2


def plane_groups():
    columns = [(x, y if x % 2 == 0 else 3 - y) for x in range(4) for y in range(4)]
    return [
        [device_of(x, y, z, c) for x, y in (columns if c == 0 else columns[::-1])]
        for z in range(4)
        for c in range(2)
    ]


def along_z(step):
    return [
        (device_of(x, y, z, c), device_of(x, y, (z + step) % 4, c))
        for x in range(4)
        for y in range(4)
        for z in range(4)
        for c in range(2)
    ]


def other_core():
    return [
        (device_of(x, y, z, c), device_of(x, y, z, 1 - c))
        for x in range(4)
        for y in range(4)
        for z in range(4)
        for c in range(2)
    ]


def send(rows, pairs):
    return lax.ppermute(rows, "d", pairs)


def exchange(rows):
    count, width = rows.shape
    return lax.all_to_all(
        rows.reshape(GROUPS, count // GROUPS, width),
        "d",
        split_axis=0,
        concat_axis=0,
        axis_index_groups=plane_groups(),
        tiled=True,
    ).reshape(count, width)


def product(a, b, dims):
    return lax.dot_general(a, b, (dims, ((), ())), preferred_element_type=jnp.float32)


def split(x):
    head = x.astype(jnp.bfloat16)
    return head, (x - head.astype(jnp.float32)).astype(jnp.bfloat16)


def dot(a, b, dims):
    return product(a[0], b[0], dims) + (product(a[0], b[1], dims) + product(a[1], b[0], dims))


def across_lanes(column):
    return jnp.broadcast_to(column, (column.shape[0], 128)).T[:1]


def add_block(left, heads, centre, rows, scratch, sums):
    count, width = sums[0].shape if sums else (left[0].shape[0] - 16, left[0].shape[1])
    head_ref, tail_ref = scratch
    at = 0
    squares = []
    for ref in rows:
        shifted = ref[...] - centre
        end = at + shifted.shape[0]
        head_ref[at:end], tail_ref[at:end] = split(shifted)
        squares.append(across_lanes(jnp.sum(shifted * shifted, axis=1, keepdims=True)))
        at = end
    square = jnp.concatenate(squares, axis=1)
    block = head_ref[...], tail_ref[...]
    crossed = dot(left, block, ((1,), (1,)))
    kernel = jnp.exp((2.0 * crossed[:count] - heads[:count] - square) * (2.0 / width))
    logits = heads[count:] + (2.0 * crossed[count:] - square) / (2.0 * variance)
    weights = jnp.exp(logits - jnp.max(logits, axis=0, keepdims=True))
    weights = weights / jnp.sum(weights, axis=0, keepdims=True)
    columns = jnp.concatenate([weights, jnp.ones_like(weights)], axis=0)
    kernel = split(kernel)
    point = dot(kernel, block, ((1,), (0,)))
    mixed = dot(kernel, split(columns), ((1,), (1,)))
    if sums:
        point, mixed = sums[0][...] + point, sums[1][...] + mixed
    return point, mixed


def first_body(own_ref, means_ref, log_ref, *refs):
    *rows, head_out, tail_out, norm_out, centre_out, point_out, mixed_out, head, tail = refs
    own = own_ref[...]
    count = own.shape[0]
    centre = jnp.mean(own, axis=0, keepdims=True)
    centre_out[...] = centre
    shifted, means = own - centre, means_ref[...] - centre
    head_out[:count], tail_out[:count] = split(shifted)
    head_out[count:], tail_out[count:] = split(means)
    norms = jnp.sum(shifted * shifted, axis=1, keepdims=True)
    mean_norms = jnp.sum(means * means, axis=1, keepdims=True)
    norm_out[:count] = jnp.broadcast_to(norms, (count, 128))
    offsets = log_ref[...] - mean_norms / (2.0 * variance)
    norm_out[count:] = jnp.broadcast_to(offsets, (offsets.shape[0], 128))
    point_out[...], mixed_out[...] = add_block(
        (head_out[...], tail_out[...]), norm_out[:, :1], centre, rows, (head, tail), None
    )


def next_body(head_ref, tail_ref, norm_ref, centre_ref, *refs):
    *rows, point_ref, mixed_ref, point_out, mixed_out, head, tail = refs
    point_out[...], mixed_out[...] = add_block(
        (head_ref[...], tail_ref[...]),
        norm_ref[:, :1],
        centre_ref[...],
        rows,
        (head, tail),
        (point_ref, mixed_ref),
    )


def last_body(members, own_ref, means_ref, head_ref, tail_ref, norm_ref, centre_ref, *refs):
    *rows, point_ref, mixed_ref, moved_out, head, tail = refs
    centre = centre_ref[...]
    point, mixed = add_block(
        (head_ref[...], tail_ref[...]),
        norm_ref[:, :1],
        centre,
        rows,
        (head, tail),
        (point_ref, mixed_ref),
    )
    own = own_ref[...]
    means = means_ref[...] - centre
    components, width = means.shape
    pulled = dot(split(mixed[:, :components]), split(means), ((1,), (0,)))
    total = mixed[:, components : components + 1]
    drift = (
        (pulled - point) / variance + 4.0 / width * ((own - centre) * total - point)
    ) / members
    moved_out[...] = own + step_size * drift


def shape_of(array):
    return jax.ShapeDtypeStruct(array.shape, array.dtype)


def call(body, operands, outs, rows):
    width = rows[0].shape[1]
    total = sum(piece.shape[0] for piece in rows)
    vmem = pl.BlockSpec(memory_space=pltpu.VMEM)
    return pl.pallas_call(
        body,
        out_shape=outs,
        in_specs=[vmem] * len(operands),
        out_specs=vmem if isinstance(outs, jax.ShapeDtypeStruct) else (vmem,) * len(outs),
        scratch_shapes=[pltpu.VMEM((total, width), jnp.bfloat16)] * 2,
        compiler_params=pltpu.CompilerParams(vmem_limit_bytes=20 * 2**20),
        cost_estimate=pl.CostEstimate(
            flops=12 * 256 * total * width,
            transcendentals=256 * total,
            bytes_accessed=4 * width * (total + 512),
        ),
    )(*operands)


def first_terms(own, means, log_weights, rows):
    count, width = own.shape
    components = means.shape[0]
    left = jax.ShapeDtypeStruct((count + components, width), jnp.bfloat16)
    outs = (
        left,
        left,
        jax.ShapeDtypeStruct((count + components, 128), jnp.float32),
        jax.ShapeDtypeStruct((1, width), jnp.float32),
        jax.ShapeDtypeStruct((count, width), jnp.float32),
        jax.ShapeDtypeStruct((count, 2 * components), jnp.float32),
    )
    out = call(first_body, [own, means, log_weights[:, None], *rows], outs, rows)
    return out[:4], out[4:]


def next_terms(left, rows, sums):
    operands = [*left, *rows, *sums]
    return call(next_body, operands, tuple(shape_of(s) for s in sums), rows)


def last_terms(own, means, left, rows, sums, members):
    operands = [own, means, *left, *rows, *sums]
    body = functools.partial(last_body, members)
    return call(body, operands, shape_of(own), rows)


def positions(batch, core):
    count = batch.shape[0]
    group = jnp.where(core == 0, batch, GROUPS - 1 - batch)
    key = group * count + lax.iota(jnp.int32, count)
    place = jnp.sum((key[None, :] < key[:, None]).astype(jnp.int32), axis=1)
    ids = lax.iota(jnp.int32, count)
    row = jnp.sum(jnp.where(place[None, :] == ids[:, None], ids[None, :], 0), axis=1)
    return place, row


def take(rows, index):
    return rows.at[index].get(mode="promise_in_bounds", unique_indices=True)


def shards(particles, batch_of, means, log_weights):
    count, _ = particles.shape
    core = (lax.axis_index("d") // 8) % 2
    above, below, beside = along_z(1), along_z(3), other_core()
    current = particles
    for iteration in range(batch_of.shape[0]):
        place, row = positions(batch_of[iteration], core)
        own = exchange(take(current, row))
        low, high = own[: count // 2], own[count // 2 :]
        near = [send(low, above), send(high, below)]
        rest = [send(high, above), send(low, below)]
        side = send(own, beside)
        far = [send(near[0], above), send(near[1], below)]
        near_side = [send(rows, beside) for rows in near]
        rest_side = [send(rows, beside) for rows in rest]
        far_side = [send(rows, beside) for rows in far]
        left, sums = first_terms(own, means, log_weights, [own, side])
        sums = next_terms(left, near + near_side, sums)
        sums = next_terms(left, rest + rest_side, sums)
        moved = last_terms(own, means, left, far + far_side, sums, 8 * count)
        current = take(exchange(moved), place)
    return current


def solution(mesh):
    flat = Mesh(mesh.devices.reshape(-1), ("d",))
    return jax.shard_map(
        shards,
        mesh=flat,
        in_specs=(P("d", None), P(None, "d"), P(), P()),
        out_specs=P("d", None),
        check_vma=False,
    )
```
